32 devices in a mesh: dom: 8 (over z, x), dir: 4 (over y, core).
Axes of the slice: x: 2, y: 2, z: 4, core: 2. Of those that a mesh axis runs over, the one named last changes fastest.
Arguments:
- x_edges: bfloat16 [65536, 128], P(('dom', 'dir')), may hold values from -6 to 6
- send_list: int32 [1024, 32], P(('dom', 'dir')), may hold values from 0 to 2048, as said below
- connectivity: int32 [6, 32768], P(None, ('dom', 'dir')), may hold values from 0 to 3071, as said below
- elem_mats: float32 [36, 32768], P(None, ('dom', 'dir'))
- elem_live: int32 [32], P(('dom', 'dir')), may hold values from 512 to 1024, as said below
- currents: bfloat16 [1024, 128, 128], P(('dom', 'dir')), may hold values from -0.1796875 to 0.1796875
- positions: bfloat16 [1024, 3, 128], P(('dom', 'dir')), may hold values from -1 to 1
- block_live: int32 [1024], P(('dom', 'dir')), may hold values from 32 to 128
- block_owner: int32 [1024], P(('dom', 'dir')), may hold values from 0 to 7, as said below
- block_leaf: int32 [1024], P(('dom', 'dir')), may hold values from 0 to 15
- cone_waves: float32 [3, 16], P(None, 'dir'), may hold values from -6 to 6
Outputs:
- interior_out: float32 [65536, 128], P(('dom', 'dir'))
- expansions: float32 [16, 16, 2, 64, 128], P('dom', 'dir')
The draws below stay inside these ranges and needn't reach their ends.
Inputs may be any that keep to these rules, and one draw needn't show every extreme that they name: `send_list`: in row a * 32 + b the used entries come first and name owned edges of a; the rest are 2048. A partition reads nothing of itself; some pair uses all 32 entries. `connectivity`: entries below 2048 are owned edges; 2048 + p * 32 + s names the s-th edge that partition p lists for this partition, and only used entries are named. `elem_live`: elements at positions from this count on are padding; some partition has all 1024. `block_owner`: among the 32 blocks of one partition at most 12 name one leaf owner; some leaf owner is named by exactly 12 blocks of every partition.
All inputs are finite; a program needn't handle non-finite values.
Results may differ from the reference program's by a relative error of at most 0.0056.
Values may be sent and summed in bfloat16 or wider, within the bound.
A program may use at most 128 MiB of HBM per device.

```python
import jax
import jax.numpy as jnp
from jax import lax

E_OWN = 2048
EL_DEV = 1024
HS = 32
NRHS = 128
BS = 128
BLK_DEV = 32
LEAVES_DEV = 16
NODES = 4
PARTITIONS = 32
OWNERS = 8
EDGES = 65536
ELEMENTS = 32768
BLOCKS = 1024
CAP = 12
LEAVES = 128
CONES = 16


def halo_counts(key):
    base_key = jax.random.fold_in(key, 7001)
    first_key, second_key, third_key, extra_key = jax.random.split(base_key, 4)
    counts = jax.random.randint(first_key, (PARTITIONS, PARTITIONS), HS // 2, HS + 1)
    rows_now = jnp.arange(PARTITIONS)[:, None]
    cols_now = jnp.arange(PARTITIONS)[None, :]
    distance = (cols_now - rows_now) % PARTITIONS
    nearby = (distance >= 1) & (distance <= 8) | (distance >= PARTITIONS - 8)
    further = jax.random.randint(extra_key, (PARTITIONS, PARTITIONS), 0, PARTITIONS) < 4
    linked = (nearby | further) & (distance != 0)
    counts = jnp.where(linked, counts, 0)
    sender = jax.random.randint(second_key, (), 0, PARTITIONS)
    stride = jax.random.randint(third_key, (), 1, PARTITIONS)
    return counts.at[sender, (sender + stride) % PARTITIONS].set(HS)


def draw_send_list(key, part):
    counts = halo_counts(key)
    entries = jax.random.randint(jax.random.fold_in(key, 7002), (PARTITIONS * PARTITIONS, HS), 0, E_OWN)
    used_slots = jnp.arange(HS)[None, :] < counts.reshape(-1)[:, None]
    return jnp.where(used_slots, entries, E_OWN).astype(jnp.int32)


def draw_connectivity(key, part):
    counts = halo_counts(key)
    incoming = counts.T
    running = jnp.cumsum(incoming, axis=1)
    totals = running[:, -1]
    keys_all = jax.random.split(jax.random.fold_in(key, 7003), 3)
    width_all = 6 * EL_DEV
    picks = jax.random.randint(keys_all[0], (PARTITIONS, width_all), 0, 1048576) % jnp.maximum(totals, 1)[:, None]
    sender = jax.vmap(lambda row_sums, wanted: jnp.searchsorted(row_sums, wanted, side='right'))(running, picks)
    sender = jnp.minimum(sender.astype(jnp.int32), PARTITIONS - 1)
    before = jnp.take_along_axis(running, sender, axis=1) - jnp.take_along_axis(incoming, sender, axis=1)
    halo_index = E_OWN + sender * HS + (picks - before)
    local_index = jax.random.randint(keys_all[1], (PARTITIONS, width_all), 0, E_OWN)
    choose_halo = (jax.random.randint(keys_all[2], (PARTITIONS, width_all), 0, 4) == 0) & (totals[:, None] > 0)
    merged = jnp.where(choose_halo, halo_index, local_index)
    return merged.reshape(PARTITIONS, 6, EL_DEV).transpose(1, 0, 2).reshape(6, PARTITIONS * EL_DEV).astype(jnp.int32)


def draw_elem_mats(key, part):
    first_key, second_key = jax.random.split(jax.random.fold_in(key, 7004), 2)
    random_part = jax.random.uniform(first_key, (6, 6, ELEMENTS), jnp.float32, -0.35, 0.35)
    symmetric = 0.5 * (random_part + random_part.transpose(1, 0, 2))
    identity = jnp.eye(6, dtype=jnp.float32)[:, :, None]
    offdiag = symmetric * (1.0 - identity)
    lifted = jnp.sum(jnp.abs(offdiag), axis=1) + jax.random.uniform(second_key, (6, ELEMENTS), jnp.float32, 0.5, 1.5)
    matrix = offdiag + identity * lifted[:, None, :]
    return (0.3 * matrix).reshape(36, ELEMENTS)


def draw_elem_live(key, part):
    first_key, second_key = jax.random.split(jax.random.fold_in(key, 7005))
    counts = jax.random.randint(first_key, (PARTITIONS,), EL_DEV // 2, EL_DEV + 1)
    fullest = jax.random.randint(second_key, (), 0, PARTITIONS)
    return counts.at[fullest].set(EL_DEV).astype(jnp.int32)


def draw_block_owner(key, part):
    base_key = jax.random.fold_in(key, 7006)
    hot_key, device_key = jax.random.split(base_key)
    hottest = jax.random.randint(hot_key, (), 0, OWNERS)
    others = BLK_DEV - CAP

    def one_device(device):
        spread_key, order_key = jax.random.split(jax.random.fold_in(device_key, device))
        places = jax.random.permutation(spread_key, (OWNERS - 1) * CAP)[:others] // CAP
        places = jnp.where(places >= hottest, places + 1, places)
        owners_now = jnp.concatenate([jnp.full((CAP,), hottest, jnp.int32), places.astype(jnp.int32)])
        return owners_now[jax.random.permutation(order_key, BLK_DEV)]
    return jax.vmap(one_device)(jnp.arange(PARTITIONS)).reshape(-1).astype(jnp.int32)


def draw_positions(key, part):
    first_key = jax.random.fold_in(jax.random.fold_in(key, 7007), 0)
    values = jax.random.uniform(first_key, (BLOCKS, 3, BS), jnp.float32, -1.0, 1.0)
    return values.astype(jnp.bfloat16)


def draw_cone_waves(key, part):
    first_key, second_key = jax.random.split(jax.random.fold_in(key, 7008))
    magnitude = jax.random.uniform(first_key, (3, CONES), jnp.float32, 5.0, 6.0)
    signs = jnp.where(jax.random.uniform(second_key, (3, CONES), jnp.float32) < 0.5, -1.0, 1.0)
    return (signs * magnitude).astype(jnp.float32)


def touch_ends(values, key, smallest, top_value):
    longest = values.shape.index(max(values.shape))
    spots = []
    for shift in (0, 1):
        where = [jax.random.randint(jax.random.fold_in(key, axis), (), 0, length) for axis, length in enumerate(values.shape)]
        where[longest] = (where[longest] + shift) % values.shape[longest]
        spots.append(tuple(where))
    return values.at[spots[0]].set(smallest).at[spots[1]].set(top_value)


def steps_of(rng, extent, cuts, smallest, high):
    def one(position, blocks):
        steps = jax.random.uniform(jax.random.fold_in(jax.random.fold_in(rng, 6), position), (blocks,), jnp.float32, smallest / len(cuts), high / len(cuts))
        return jnp.repeat(jnp.exp(steps), extent[position] // blocks).reshape((-1,) + (1,) * (len(extent) - position - 1))

    level = one(*cuts[0])
    for cut in cuts[1:]:
        level = level * one(*cut)
    return level


def gaussian(stream_key, shape, width, bound, shards=(), held_as=jnp.bfloat16):
    level = steps_of(stream_key, shape, shards, -0.22, 0.18) if shards else 1.0
    array = jax.random.normal(stream_key, shape, jnp.float32) * width * level
    return jnp.minimum(jnp.maximum(array, -bound), bound).astype(held_as)


def setup_inputs(seed: int = 0) -> dict:
    seeds = jax.random.split(jax.random.key(seed), 12)
    x_edges = gaussian(seeds[0], (EDGES, NRHS), 1.0, 6.0, ((0, 32),))
    send_list = draw_send_list(jax.random.fold_in(seeds[11], 71), 0)
    connectivity = draw_connectivity(jax.random.fold_in(seeds[11], 71), 0)
    elem_mats = draw_elem_mats(jax.random.fold_in(seeds[11], 71), 0)
    elem_live = draw_elem_live(jax.random.fold_in(seeds[11], 71), 0)
    currents = gaussian(seeds[5], (BLOCKS, BS, NRHS), 0.03, 0.1796875, ((0, 32),))
    positions = draw_positions(jax.random.fold_in(seeds[11], 71), 0)
    block_live = touch_ends(jax.random.randint(seeds[7], (BLOCKS,), BS // 4, BS + 1), jax.random.fold_in(seeds[7], 1), BS // 4, BS).astype(jnp.int32)
    block_owner = draw_block_owner(jax.random.fold_in(seeds[11], 71), 0)
    block_leaf = touch_ends(jax.random.randint(seeds[9], (BLOCKS,), 0, LEAVES_DEV), jax.random.fold_in(seeds[9], 1), 0, LEAVES_DEV - 1).astype(jnp.int32)
    cone_waves = draw_cone_waves(jax.random.fold_in(seeds[11], 71), 0)
    return {"x_edges": x_edges, "send_list": send_list, "connectivity": connectivity, "elem_mats": elem_mats, "elem_live": elem_live, "currents": currents, "positions": positions, "block_live": block_live, "block_owner": block_owner, "block_leaf": block_leaf, "cone_waves": cone_waves}


def cheb_points():
    node_order = jnp.arange(NODES).astype(jnp.float32)
    return jnp.cos((2.0 * node_order + 1.0) * (jnp.pi / (2.0 * NODES)))


def lagrange(points):
    node_values = cheb_points()
    rows_out = []
    for target in range(NODES):
        product = jnp.ones_like(points)
        for other_node in range(NODES):
            if other_node != target:
                product = product * (points - node_values[other_node]) / (node_values[target] - node_values[other_node])
        rows_out.append(product)
    return jnp.stack(rows_out, axis=-2)


def tensor_basis(coords):
    first = lagrange(coords[..., 0, :])
    second = lagrange(coords[..., 1, :])
    third = lagrange(coords[..., 2, :])
    joined = first[..., :, None, None, :] * second[..., None, :, None, :] * third[..., None, None, :, :]
    return joined.reshape(coords.shape[:-2] + (NODES ** 3, coords.shape[-1]))


def node_coords():
    ladder = jnp.arange(NODES ** 3)
    digits = jnp.stack([ladder // (NODES * NODES), (ladder // NODES) % NODES, ladder % NODES]).astype(jnp.float32)
    return jnp.cos((2.0 * digits + 1.0) * (jnp.pi / (2.0 * NODES)))


def wave_phase(waves, coords):
    return (waves[0][:, None] * coords[..., None, 0, :] + waves[1][:, None] * coords[..., None, 1, :]
            + waves[2][:, None] * coords[..., None, 2, :])


def m2m_tables(waves):
    octant = jnp.arange(8)
    shifts = jnp.stack([octant // 4, (octant // 2) % 2, octant % 2], axis=1).astype(jnp.float32) - 0.5
    points = shifts[:, :, None] + 0.5 * cheb_points()[None, None, :]
    weights = lagrange(points)
    first = weights[:, 0]
    second = weights[:, 1]
    third = weights[:, 2]
    joined = first[:, :, None, None, :, None, None] * second[:, None, :, None, None, :, None] * third[:, None, None, :, None, None, :]
    square = NODES ** 3
    joined = joined.reshape(8, square, square)
    child = shifts[:, :, None] + 0.5 * node_coords()[None]
    spread = child[:, :, None, :] - node_coords()[None, :, :, None]
    psi = 2.0 * (waves[0][:, None, None, None] * spread[None, :, 0] + waves[1][:, None, None, None] * spread[None, :, 1]
                 + waves[2][:, None, None, None] * spread[None, :, 2])
    table_real = (joined[None] * jnp.cos(psi)).astype(jnp.bfloat16)
    table_imag = (-joined[None] * jnp.sin(psi)).astype(jnp.bfloat16)
    return table_real, table_imag


def interior_product(x_edges, send_list, connectivity, elem_mats, elem_live):
    total_rows = x_edges.shape[0]
    columns = x_edges.shape[1]

    def one_part(accumulated, device):
        local_links = lax.dynamic_slice_in_dim(connectivity, device * EL_DEV, EL_DEV, 1)
        matrices = lax.dynamic_slice_in_dim(elem_mats, device * EL_DEV, EL_DEV, 1)
        offset = jnp.maximum(local_links - E_OWN, 0)
        sender = offset // HS
        listed = send_list[sender * PARTITIONS + device, offset % HS]
        global_rows = jnp.where(local_links < E_OWN, device * E_OWN + local_links, sender * E_OWN + listed).astype(jnp.int32)
        gathered = x_edges[global_rows]
        live_mask = (jnp.arange(EL_DEV) < elem_live[device])[:, None]
        term_list = []
        for row_index in range(6):
            summed = jnp.zeros((EL_DEV, columns), jnp.float32)
            for col_index in range(6):
                summed = summed + matrices[row_index * 6 + col_index][:, None] * gathered[col_index].astype(jnp.float32)
            term_list.append(jnp.where(live_mask, summed, jnp.zeros_like(summed)))
        stacked = jnp.stack(term_list).reshape(6 * EL_DEV, columns)
        return accumulated.at[global_rows.reshape(-1)].add(stacked), None

    initial = jnp.zeros((total_rows, columns), jnp.float32)
    result, unused = lax.scan(one_part, initial, jnp.arange(PARTITIONS, dtype=jnp.int32))
    return result


def boundary_product(currents, positions, block_live, block_owner, block_leaf, cone_waves):
    cone_total = cone_waves.shape[1]
    columns = currents.shape[2]
    square = NODES ** 3
    live_mask = jnp.arange(BS)[None, :] < block_live[:, None]
    masked = jnp.where(live_mask[:, :, None], currents, jnp.zeros_like(currents))
    leaf_index = (block_owner * LEAVES_DEV + block_leaf).astype(jnp.int32)
    batches = BLOCKS // 128

    def one_batch(carry, inputs):
        real_sum, imag_sum = carry
        blocks_now, coords, leaves = inputs
        coords_wide = coords.astype(jnp.float32)
        basis_now = tensor_basis(coords_wide)
        phase_now = wave_phase(cone_waves, coords_wide)
        real_w = (basis_now[:, None] * jnp.cos(phase_now)[:, :, None, :]).astype(jnp.bfloat16)
        imag_w = (-basis_now[:, None] * jnp.sin(phase_now)[:, :, None, :]).astype(jnp.bfloat16)
        block_data = blocks_now.astype(jnp.float32)
        real_part = jnp.einsum("gcqb,gbn->gcqn", real_w.astype(jnp.float32), block_data).astype(jnp.bfloat16)
        imag_part = jnp.einsum("gcqb,gbn->gcqn", imag_w.astype(jnp.float32), block_data).astype(jnp.bfloat16)
        real_sum = real_sum.at[leaves].add(real_part.astype(jnp.float32))
        imag_sum = imag_sum.at[leaves].add(imag_part.astype(jnp.float32))
        return (real_sum, imag_sum), None

    empty = jnp.zeros((LEAVES, cone_total, square, columns), jnp.float32)
    inputs = (masked.reshape(batches, 128, BS, columns), positions.reshape(batches, 128, 3, BS), leaf_index.reshape(batches, 128))
    sums, unused = lax.scan(one_batch, (empty, empty), inputs)
    real_sum, imag_sum = sums
    node_phase = wave_phase(cone_waves, node_coords())
    cosine = jnp.cos(node_phase)[None, :, :, None]
    sine_part = jnp.sin(node_phase)[None, :, :, None]
    leaf_real = (cosine * real_sum - sine_part * imag_sum).astype(jnp.bfloat16)
    leaf_imag = (cosine * imag_sum + sine_part * real_sum).astype(jnp.bfloat16)
    table_real, table_imag = m2m_tables(cone_waves)
    child_real = leaf_real.reshape(LEAVES // 8, 8, cone_total, square, columns).astype(jnp.float32)
    child_imag = leaf_imag.reshape(LEAVES // 8, 8, cone_total, square, columns).astype(jnp.float32)
    wide_real = table_real.astype(jnp.float32)
    wide_imag = table_imag.astype(jnp.float32)
    parent_real = jnp.einsum("cops,xocsn->xcpn", wide_real, child_real) - jnp.einsum("cops,xocsn->xcpn", wide_imag, child_imag)
    parent_imag = jnp.einsum("cops,xocsn->xcpn", wide_real, child_imag) + jnp.einsum("cops,xocsn->xcpn", wide_imag, child_real)
    return jnp.stack([parent_real, parent_imag], axis=2)


def reference(x_edges, send_list, connectivity, elem_mats, elem_live, currents, positions, block_live, block_owner, block_leaf, cone_waves):
    interior_out = interior_product(x_edges, send_list, connectivity, elem_mats, elem_live)
    expansions = boundary_product(currents, positions, block_live, block_owner, block_leaf, cone_waves)
    return (interior_out, expansions)
```

```python
import jax
import jax.numpy as jnp
from jax import lax
from jax.experimental import pallas as pl
from jax.experimental.pallas import tpu as pltpu
from jax.sharding import PartitionSpec as P

LEAVES_DEV = 16
NODES = 4


def cheb_points():
    node_order = jnp.arange(NODES).astype(jnp.float32)
    return jnp.cos((2.0 * node_order + 1.0) * (jnp.pi / (2.0 * NODES)))


def lagrange(points):
    node_values = cheb_points()
    rows_out = []
    for target in range(NODES):
        product = jnp.ones_like(points)
        for other_node in range(NODES):
            if other_node != target:
                product = (
                    product
                    * (points - node_values[other_node])
                    / (node_values[target] - node_values[other_node])
                )
        rows_out.append(product)
    return jnp.stack(rows_out, axis=-2)


def tensor_basis(coords):
    first = lagrange(coords[..., 0, :])
    second = lagrange(coords[..., 1, :])
    third = lagrange(coords[..., 2, :])
    joined = (
        first[..., :, None, None, :] * second[..., None, :, None, :] * third[..., None, None, :, :]
    )
    return joined.reshape(coords.shape[:-2] + (NODES**3, coords.shape[-1]))


def node_coords():
    ladder = jnp.arange(NODES**3)
    digits = jnp.stack([ladder // (NODES * NODES), ladder // NODES % NODES, ladder % NODES]).astype(
        jnp.float32
    )
    return jnp.cos((2.0 * digits + 1.0) * (jnp.pi / (2.0 * NODES)))


def wave_phase(waves, coords):
    return (
        waves[0][:, None] * coords[..., None, 0, :]
        + waves[1][:, None] * coords[..., None, 1, :]
        + waves[2][:, None] * coords[..., None, 2, :]
    )


def m2m_tables(waves):
    octant = jnp.arange(8)
    shifts = jnp.stack([octant // 4, octant // 2 % 2, octant % 2], axis=1).astype(jnp.float32) - 0.5
    points = shifts[:, :, None] + 0.5 * cheb_points()[None, None, :]
    weights = lagrange(points)
    first = weights[:, 0]
    second = weights[:, 1]
    third = weights[:, 2]
    joined = (
        first[:, :, None, None, :, None, None]
        * second[:, None, :, None, None, :, None]
        * third[:, None, None, :, None, None, :]
    )
    square = NODES**3
    joined = joined.reshape(8, square, square)
    child = shifts[:, :, None] + 0.5 * node_coords()[None]
    spread = child[:, :, None, :] - node_coords()[None, :, :, None]
    psi = 2.0 * (
        waves[0][:, None, None, None] * spread[None, :, 0]
        + waves[1][:, None, None, None] * spread[None, :, 1]
        + waves[2][:, None, None, None] * spread[None, :, 2]
    )
    table_real = (joined[None] * jnp.cos(psi)).astype(jnp.bfloat16)
    table_imag = (-joined[None] * jnp.sin(psi)).astype(jnp.bfloat16)
    return (table_real, table_imag)


def pack_slots(owners, dest_count, capacity, members):
    matches = (owners[:, None] == jnp.arange(dest_count)[None, :]).astype(jnp.int32)
    ranking = jnp.sum((jnp.cumsum(matches, axis=0) - matches) * matches, axis=1)
    slot_index = owners * capacity + ranking
    source_row = (
        jnp.full((dest_count * capacity,), owners.shape[0], jnp.int32)
        .at[slot_index]
        .set(jnp.arange(owners.shape[0], dtype=jnp.int32))
    )
    padded = [
        jnp.concatenate([member, jnp.zeros((1,) + member.shape[1:], member.dtype)])
        for member in members
    ]
    return tuple((array_now[source_row] for array_now in padded))


def interior_part(x_edges, send_list, connectivity, elem_mats, elem_live):
    owned_rows, columns = x_edges.shape
    partitions, slot_width = send_list.shape
    element_count = connectivity.shape[1]
    padded = jnp.concatenate([x_edges, jnp.zeros((1, columns), x_edges.dtype)])
    outgoing = padded[send_list]
    received = lax.all_to_all(outgoing, ("dom", "dir"), split_axis=0, concat_axis=0, tiled=True)
    edge_table = jnp.concatenate([x_edges, received.reshape(partitions * slot_width, columns)])
    gathered = edge_table[connectivity]
    live_mask = (jnp.arange(element_count) < elem_live[0])[:, None]
    term_list = []
    for row_index in range(6):
        summed = jnp.zeros((element_count, columns), jnp.float32)
        for col_index in range(6):
            summed = summed + elem_mats[row_index * 6 + col_index][:, None] * gathered[col_index]
        term_list.append(jnp.where(live_mask, summed, jnp.zeros_like(summed)))
    stacked = jnp.stack(term_list).reshape(6 * element_count, columns)
    assembled = jax.ops.segment_sum(
        stacked, connectivity.reshape(-1), num_segments=owned_rows + partitions * slot_width
    )
    back_terms = assembled[owned_rows:]
    returned = lax.all_to_all(
        back_terms.reshape(partitions, slot_width, columns),
        ("dom", "dir"),
        split_axis=0,
        concat_axis=0,
        tiled=True,
    )
    folded = jax.ops.segment_sum(
        returned.reshape(-1, columns), send_list.reshape(-1), num_segments=owned_rows + 1
    )
    return assembled[:owned_rows] + folded[:owned_rows]


def block_sums(leaf_ids, factors, blocks, cone_count):
    block_count, block_size, columns = blocks.shape
    rows = factors.shape[1]
    plane = NODES * NODES
    height = 2 * cone_count * NODES**3
    group = next(size for size in (8, 4, 2, 1) if block_count % size == 0)

    def kernel(leaf_ref, factor_ref, block_ref, out_ref):
        step = pl.program_id(0)

        @pl.when(step == 0)
        def _():
            out_ref[...] = jnp.zeros_like(out_ref)

        for g in range(group):
            pairs = factor_ref[g, :plane, :]
            first = factor_ref[g, plane : plane + NODES, :]
            pieces = []
            for wave in range(2 * cone_count):
                at = plane + NODES + wave
                scaled = first * factor_ref[g, at : at + 1, :]
                for digit in range(NODES):
                    pieces.append((scaled[digit : digit + 1] * pairs).astype(jnp.bfloat16))
            weights = jnp.concatenate(pieces, axis=0)
            product = jnp.dot(weights, block_ref[g], preferred_element_type=jnp.float32)
            leaf = leaf_ref[step * group + g]
            out_ref[leaf] += product

    return pl.pallas_call(
        kernel,
        out_shape=jax.ShapeDtypeStruct((LEAVES_DEV, height, columns), jnp.float32),
        grid_spec=pltpu.PrefetchScalarGridSpec(
            num_scalar_prefetch=1,
            grid=(block_count // group,),
            in_specs=[
                pl.BlockSpec((group, rows, block_size), lambda i, leaf: (i, 0, 0)),
                pl.BlockSpec((group, block_size, columns), lambda i, leaf: (i, 0, 0)),
            ],
            out_specs=pl.BlockSpec((LEAVES_DEV, height, columns), lambda i, leaf: (0, 0, 0)),
        ),
        cost_estimate=pl.CostEstimate(
            flops=2 * block_count * height * block_size * columns,
            bytes_accessed=block_count * block_size * (rows * 4 + columns * 2),
            transcendentals=0,
        ),
    )(leaf_ids, factors, blocks)


def expand_leaves(arrived_blocks, arrived_meta, waves):
    columns = arrived_blocks.shape[2]
    cone_count = waves.shape[1]
    square = NODES**3
    leaf_ids = arrived_meta[:, 3, 0].astype(jnp.int32)
    coords = arrived_meta[:, :3].astype(jnp.float32)
    second = lagrange(coords[:, 1])
    third = lagrange(coords[:, 2])
    pairs = (second[:, :, None] * third[:, None, :]).reshape(
        coords.shape[0], NODES * NODES, coords.shape[2]
    )
    phase = wave_phase(waves, coords)
    factors = jnp.concatenate(
        [pairs, lagrange(coords[:, 0]), jnp.cos(phase), -jnp.sin(phase)], axis=1
    )
    sums = block_sums(leaf_ids, factors, arrived_blocks, cone_count).reshape(
        LEAVES_DEV, 2, cone_count, square, columns
    )
    real_sum, imag_sum = sums[:, 0], sums[:, 1]
    node_phase = wave_phase(waves, node_coords())
    cosine = jnp.cos(node_phase)[None, :, :, None]
    sine_part = jnp.sin(node_phase)[None, :, :, None]
    leaf_real = (cosine * real_sum - sine_part * imag_sum).astype(jnp.bfloat16)
    leaf_imag = (cosine * imag_sum + sine_part * real_sum).astype(jnp.bfloat16)
    table_real, table_imag = m2m_tables(waves)
    child_real = leaf_real.reshape(LEAVES_DEV // 8, 8, cone_count, square, columns)
    child_imag = leaf_imag.reshape(LEAVES_DEV // 8, 8, cone_count, square, columns)
    parent_real = jnp.einsum(
        "cops,xocsn->xcpn", table_real, child_real, preferred_element_type=jnp.float32
    ) - jnp.einsum("cops,xocsn->xcpn", table_imag, child_imag, preferred_element_type=jnp.float32)
    parent_imag = jnp.einsum(
        "cops,xocsn->xcpn", table_real, child_imag, preferred_element_type=jnp.float32
    ) + jnp.einsum("cops,xocsn->xcpn", table_imag, child_real, preferred_element_type=jnp.float32)
    return jnp.stack([parent_real, parent_imag], axis=2)


def boundary_part(currents, positions, block_live, block_owner, block_leaf, cone_waves):
    block_count, block_size, columns = currents.shape
    dom_count = lax.axis_size("dom")
    capacity = 3 * block_count // dom_count
    live_mask = jnp.arange(block_size)[None, :] < block_live[:, None]
    masked = jnp.where(live_mask[:, :, None], currents, jnp.zeros_like(currents))
    leaf_row = jnp.broadcast_to(
        block_leaf.astype(jnp.bfloat16)[:, None, None], (block_count, 1, block_size)
    )
    described = jnp.concatenate([positions, leaf_row], axis=1)
    packed_blocks, packed_meta = pack_slots(block_owner, dom_count, capacity, (masked, described))
    owner_blocks, owner_meta = (
        lax.all_to_all(packed_blocks, "dom", split_axis=0, concat_axis=0, tiled=True),
        lax.all_to_all(packed_meta, "dom", split_axis=0, concat_axis=0, tiled=True),
    )
    arrived_blocks, arrived_meta = (
        lax.all_gather(owner_blocks, "dir", axis=0, tiled=True),
        lax.all_gather(owner_meta, "dir", axis=0, tiled=True),
    )
    parents = expand_leaves(arrived_blocks, arrived_meta, cone_waves)
    return parents


def shards(
    x_edges,
    send_list,
    connectivity,
    elem_mats,
    elem_live,
    currents,
    positions,
    block_live,
    block_owner,
    block_leaf,
    cone_waves,
):
    interior_out = interior_part(x_edges, send_list, connectivity, elem_mats, elem_live)
    expansions = boundary_part(currents, positions, block_live, block_owner, block_leaf, cone_waves)
    return (interior_out, expansions)


def solution(mesh):
    placed = (
        P(("dom", "dir"), None),
        P(("dom", "dir"), None),
        P(None, ("dom", "dir")),
        P(None, ("dom", "dir")),
        P(("dom", "dir")),
        P(("dom", "dir"), None, None),
        P(("dom", "dir"), None, None),
        P(("dom", "dir")),
        P(("dom", "dir")),
        P(("dom", "dir")),
        P(None, "dir"),
    )
    return jax.shard_map(
        shards,
        mesh=mesh,
        in_specs=placed,
        out_specs=(P(("dom", "dir"), None), P("dom", "dir", None, None, None)),
        check_vma=False,
    )
```
